32 devices in a mesh: dp: 8 (over y, x, core), tm: 4 (over z).
Axes of the slice: x: 2, y: 2, z: 4, core: 2. Of those that a mesh axis runs over, the one named last changes fastest.
Arguments:
- audio: float32 [24, 8, 1024], P('dp', None, 'tm'), may hold values from -3.15 to 3.15, as said below
- mel_frames: bfloat16 [24, 1024, 640], P('dp', 'tm'), may hold values from -6 to 6
- start_weight: float32 [4, 512], replicated, may hold values from -3 to 3
- input_weight: bfloat16 [2, 3, 512, 1024], replicated, may hold values from -0.15625 to 0.15625
- cond_weight: bfloat16 [2, 640, 1024], replicated, may hold values from -0.25 to 0.25
- res_weight: bfloat16 [1, 512, 1024], replicated, may hold values from -0.25 to 0.25
- last_weight: bfloat16 [512, 512], replicated, may hold values from -0.25 to 0.25
- end_weight: bfloat16 [512, 8], replicated, may hold values from -0.25 to 0.25
Outputs:
- latent: float32 [24, 4, 1024], P('dp', None, 'tm')
- audio_grad: float32 [24, 8, 1024], P('dp', None, 'tm')
- batch_loss: float32 [], replicated
- input_weight_grad: float32 [2, 3, 512, 1024], P(None, None, 'dp', 'tm')
- cond_weight_grad: float32 [2, 640, 1024], P(None, 'dp', 'tm')
- res_weight_grad: float32 [1, 512, 1024], P(None, 'dp', 'tm')
- last_weight_grad: float32 [512, 512], replicated
- end_weight_grad: float32 [512, 8], replicated
- start_weight_grad: float32 [4, 512], replicated
The draws below stay inside these ranges and needn't reach their ends.
Inputs may be any that keep to these rules, and one draw needn't show every extreme that they name: `audio`: audio samples.
All inputs are finite; a program needn't handle non-finite values.
Results may differ from the reference program's by a relative error of at most 0.015.
Values may be sent and summed in bfloat16 or wider, within the bound.
A program may use at most 128 MiB of HBM per device.

```python
import jax
import jax.numpy as jnp
from jax import lax

C = 512
COND = 640
GROUP = 8
TAPS = 3
LAYERS = 2
HALF = 4
CLIPS = 24
FRAMES = 1024


def draw_audio(key, part):
    first_key = jax.random.fold_in(key, 0)
    clip_rise = 1.0 + 2.0 * jnp.arange(CLIPS, dtype=jnp.float32) / max(CLIPS - 1, 1)
    time_rise = 1.0 + 2.0 * jnp.arange(FRAMES, dtype=jnp.float32) / max(FRAMES - 1, 1)
    envelope = clip_rise[:, None, None] * time_rise[None, None, :]
    values = 0.1 * jnp.clip(jax.random.normal(first_key, (CLIPS, GROUP, FRAMES), jnp.float32), -3.5, 3.5)
    return values * envelope


def steps_of(rng, shape, shards, low, top_value):
    factor_of = 1.0
    for axis_at, parts in shards:
        steps = jax.random.uniform(jax.random.fold_in(jax.random.fold_in(rng, 6), axis_at), (parts,), jnp.float32, low / len(shards), top_value / len(shards))
        factor_of = factor_of * jnp.repeat(jnp.exp(steps), shape[axis_at] // parts).reshape((-1,) + (1,) * (len(shape) - 1 - axis_at))
    return factor_of


def gaussian(key, dims, scale, most, cuts=(), held_as=jnp.bfloat16):
    level = steps_of(key, dims, cuts, -0.22, 0.18) if cuts else 1.0
    drawn = jax.random.normal(key, dims, jnp.float32) * scale * level
    return jnp.minimum(jnp.maximum(drawn, -most), most).astype(held_as)


def setup_inputs(seed: int = 0) -> dict:
    seeds = jax.random.split(jax.random.key(seed), 9)
    audio = draw_audio(jax.random.fold_in(seeds[8], 71), 0)
    mel_frames = gaussian(seeds[1], (CLIPS, FRAMES, COND), 1.0, 6.0, ((0, 8), (1, 4)))
    start_weight = gaussian(seeds[2], (HALF, C), HALF ** -0.5, 3.0, (), jnp.float32)
    input_weight = gaussian(seeds[3], (LAYERS, TAPS, C, 2 * C), (TAPS * C) ** -0.5, 0.15625)
    cond_weight = gaussian(seeds[4], (LAYERS, COND, 2 * C), COND ** -0.5, 0.25)
    res_weight = gaussian(seeds[5], (LAYERS - 1, C, 2 * C), C ** -0.5, 0.25)
    last_weight = gaussian(seeds[6], (C, C), C ** -0.5, 0.25)
    end_weight = gaussian(seeds[7], (C, GROUP), C ** -0.5, 0.25)
    return {"audio": audio, "mel_frames": mel_frames, "start_weight": start_weight, "input_weight": input_weight, "cond_weight": cond_weight, "res_weight": res_weight, "last_weight": last_weight, "end_weight": end_weight}


highest = lax.Precision.HIGHEST


def gated_unit(pre_act, channels):
    return jnp.tanh(pre_act[:, :channels]) * jax.nn.sigmoid(pre_act[:, channels:])


def gated_back(pre_act, upstream, channels):
    tangent = jnp.tanh(pre_act[:, :channels])
    switch = jax.nn.sigmoid(pre_act[:, channels:])
    return jnp.concatenate([upstream * (1.0 - tangent * tangent) * switch, upstream * tangent * switch * (1.0 - switch)], axis=1)


def dilated(padded, weight, spread, length):
    summed = jnp.zeros((length, weight.shape[2]), jnp.float32)
    for tap_index in range(weight.shape[0]):
        window = padded[tap_index * spread:tap_index * spread + length]
        summed = summed + jnp.dot(window, weight[tap_index], preferred_element_type=jnp.float32)
    return summed


def dilated_back(padded_grad, weight, spread, length):
    taps = weight.shape[0]
    summed = jnp.zeros((length, weight.shape[1]), jnp.float32)
    for tap_index in range(taps):
        offset = (taps - 1 - tap_index) * spread
        window = padded_grad[offset:offset + length]
        summed = summed + jnp.dot(window, weight[tap_index].T, preferred_element_type=jnp.float32)
    return summed


def clip_work(audio_clip, mel_clip, weights, scale_inv):
    start_weight, input_weight, cond_weight, res_weight, last_weight, end_weight = weights
    half_group = audio_clip.shape[0] // 2
    length = audio_clip.shape[1]
    channels = start_weight.shape[1]
    taps = input_weight.shape[1]
    first_half = audio_clip[:half_group].T
    second_half = audio_clip[half_group:].T
    hidden = jnp.dot(first_half, start_weight, precision=highest)
    skip_sum = jnp.zeros((length, channels), jnp.float32)
    stored = []
    for layer_index in range(LAYERS):
        spread = 2 ** layer_index
        state_b = hidden.astype(jnp.bfloat16)
        padded = jnp.pad(state_b, ((spread, spread), (0, 0)))
        pre_act = dilated(padded, input_weight[layer_index], spread, length) + jnp.dot(mel_clip, cond_weight[layer_index], preferred_element_type=jnp.float32)
        gated_out = gated_unit(pre_act, channels).astype(jnp.bfloat16)
        stored.append((padded, pre_act, gated_out))
        if layer_index < LAYERS - 1:
            mixed = jnp.dot(gated_out, res_weight[layer_index], preferred_element_type=jnp.float32)
            hidden = hidden + mixed[:, :channels]
            skip_sum = skip_sum + mixed[:, channels:]
        else:
            skip_sum = skip_sum + jnp.dot(gated_out, last_weight, preferred_element_type=jnp.float32)
    skip_b = skip_sum.astype(jnp.bfloat16)
    outputs = jnp.dot(skip_b, end_weight, preferred_element_type=jnp.float32)
    log_scale = outputs[:, :half_group]
    shift_term = outputs[:, half_group:]
    growth = jnp.exp(log_scale)
    latent_rows = growth * second_half + shift_term
    loss_part = (0.5 * jnp.sum(first_half * first_half) + 0.5 * jnp.sum(latent_rows * latent_rows) - jnp.sum(log_scale)) * scale_inv
    grad_out = jnp.concatenate([(latent_rows * growth * second_half - 1.0) * scale_inv, latent_rows * scale_inv], axis=1).astype(jnp.bfloat16)
    end_grad = jnp.dot(skip_b.T, grad_out, preferred_element_type=jnp.float32)
    skip_back = jnp.dot(grad_out, end_weight.T, preferred_element_type=jnp.float32).astype(jnp.bfloat16)
    state_back = jnp.zeros((length, channels), jnp.float32)
    in_grads = [None] * LAYERS
    cond_grads = [None] * LAYERS
    res_grads = [None] * (LAYERS - 1)
    last_grad = None
    for layer_index in reversed(range(LAYERS)):
        spread = 2 ** layer_index
        padded, pre_act, gated_out = stored[layer_index]
        if layer_index == LAYERS - 1:
            act_back = jnp.dot(skip_back, last_weight.T, preferred_element_type=jnp.float32)
            last_grad = jnp.dot(gated_out.T, skip_back, preferred_element_type=jnp.float32)
        else:
            joined = jnp.concatenate([state_back.astype(jnp.bfloat16), skip_back], axis=1)
            act_back = jnp.dot(joined, res_weight[layer_index].T, preferred_element_type=jnp.float32)
            res_grads[layer_index] = jnp.dot(gated_out.T, joined, preferred_element_type=jnp.float32)
        pre_back = gated_back(pre_act, act_back, channels).astype(jnp.bfloat16)
        in_grads[layer_index] = jnp.stack([jnp.dot(padded[tap_index * spread:tap_index * spread + length].T, pre_back, preferred_element_type=jnp.float32) for tap_index in range(taps)])
        cond_grads[layer_index] = jnp.dot(mel_clip.T, pre_back, preferred_element_type=jnp.float32)
        grad_pad = jnp.pad(pre_back, ((spread, spread), (0, 0)))
        state_back = state_back + dilated_back(grad_pad, input_weight[layer_index], spread, length)
    start_grad = jnp.dot(first_half.T, state_back, precision=highest)
    first_back = jnp.dot(state_back, start_weight.T, precision=highest) + first_half * scale_inv
    audio_back = jnp.concatenate([first_back, latent_rows * growth * scale_inv], axis=1).T
    grads = (jnp.stack(in_grads), jnp.stack(cond_grads), jnp.stack(res_grads), last_grad, end_grad, start_grad)
    return latent_rows.T, audio_back, loss_part, grads


def reference(audio, mel_frames, start_weight, input_weight, cond_weight, res_weight, last_weight, end_weight):
    weights = (start_weight, input_weight, cond_weight, res_weight, last_weight, end_weight)
    scale_inv = 1.0 / CLIPS
    channels = start_weight.shape[1]
    initial = (jnp.zeros((), jnp.float32),
               jnp.zeros(input_weight.shape, jnp.float32),
               jnp.zeros(cond_weight.shape, jnp.float32),
               jnp.zeros(res_weight.shape, jnp.float32),
               jnp.zeros((channels, channels), jnp.float32),
               jnp.zeros(end_weight.shape, jnp.float32),
               jnp.zeros(start_weight.shape, jnp.float32))

    def clip_step(running, clip_pair):
        audio_clip, mel_clip = clip_pair
        latent_clip, audio_back, loss_part, grads = clip_work(audio_clip, mel_clip, weights, scale_inv)
        running = jax.tree.map(lambda held, current: held + current, running, (loss_part,) + grads)
        return running, (latent_clip, audio_back)

    summed_all, stacked = lax.scan(clip_step, initial, (audio, mel_frames))
    batch_loss, in_grad, cond_grad, res_grad, last_grad, end_grad, start_grad = summed_all
    return stacked[0], stacked[1], batch_loss, in_grad, cond_grad, res_grad, last_grad, end_grad, start_grad
```

```python
import jax
import jax.numpy as jnp
from jax import lax
from jax.experimental.layout import Layout, with_layout_constraint
from jax.sharding import PartitionSpec as P

highest = lax.Precision.HIGHEST


def with_halo(block, sides, width):
    for axis, dim in sides:
        count = lax.axis_size(axis)
        forward = [(i, i + 1) for i in range(count - 1)]
        backward = [(target, source) for source, target in forward]
        low = lax.ppermute(
            lax.slice_in_dim(block, block.shape[dim] - width, None, axis=dim), axis, forward
        )
        high = lax.ppermute(lax.slice_in_dim(block, 0, width, axis=dim), axis, backward)
        block = jnp.concatenate([low, block, high], axis=dim)
    return block


def gated_unit(pre_act, channels):
    return jnp.tanh(pre_act[..., :channels]) * jax.nn.sigmoid(pre_act[..., channels:])


def gated_back(pre_act, upstream, channels):
    tangent = jnp.tanh(pre_act[..., :channels])
    switch = jax.nn.sigmoid(pre_act[..., channels:])
    return jnp.concatenate(
        [
            upstream * (1.0 - tangent * tangent) * switch,
            upstream * tangent * switch * (1.0 - switch),
        ],
        axis=-1,
    )


def project(values, weight):
    return jnp.einsum("cti,io->cto", values, weight, preferred_element_type=jnp.float32)


def dilated(padded, weight, spread, length):
    summed = None
    for tap_index in range(weight.shape[0]):
        window = padded[:, tap_index * spread : tap_index * spread + length]
        tap_term = project(window, weight[tap_index])
        summed = tap_term if summed is None else summed + tap_term
    return summed


def dilated_back(padded_grad, weight, spread, length):
    taps = weight.shape[0]
    summed = None
    for tap_index in range(taps):
        offset = (taps - 1 - tap_index) * spread
        window = padded_grad[:, offset : offset + length]
        tap_term = jnp.einsum(
            "cto,io->cti", window, weight[tap_index], preferred_element_type=jnp.float32
        )
        summed = tap_term if summed is None else summed + tap_term
    return summed


def shards(
    audio, mel_frames, start_weight, input_weight, cond_weight, res_weight, last_weight, end_weight
):
    clips_dev, group_size, frames_dev = audio.shape
    half_group = group_size // 2
    channels = start_weight.shape[1]
    layers = input_weight.shape[0]
    taps = input_weight.shape[1]
    scale_inv = 1.0 / (clips_dev * lax.axis_size("dp"))
    first_half = jnp.transpose(audio[:, :half_group], (0, 2, 1))
    second_half = jnp.transpose(audio[:, half_group:], (0, 2, 1))
    stored = []
    skip_sum = jnp.zeros((clips_dev, frames_dev, channels), jnp.float32)
    hidden = jnp.einsum("cth,hk->ctk", first_half, start_weight, precision=highest)
    for layer_index in range(layers):
        spread = 2**layer_index
        padded = with_halo(hidden.astype(jnp.bfloat16), (("tm", 1),), spread)
        pre_act = dilated(padded, input_weight[layer_index], spread, frames_dev) + project(
            mel_frames, cond_weight[layer_index]
        )
        gated_out = gated_unit(pre_act, channels).astype(jnp.bfloat16)
        stored.append((padded, pre_act, gated_out))
        if layer_index < layers - 1:
            mixed = project(gated_out, res_weight[layer_index])
            hidden = hidden + mixed[..., :channels]
            skip_sum = mixed[..., channels:]
        else:
            skip_sum = skip_sum + project(gated_out, last_weight)
    skip_b = skip_sum.astype(jnp.bfloat16)
    outputs = project(skip_b, end_weight)
    log_scale = outputs[..., :half_group]
    shift_term = outputs[..., half_group:]
    growth = jnp.exp(log_scale)
    latent_rows = growth * second_half + shift_term
    local_loss = (
        0.5 * jnp.sum(first_half * first_half)
        + 0.5 * jnp.sum(latent_rows * latent_rows)
        - jnp.sum(log_scale)
    ) * scale_inv
    grad_out = jnp.concatenate(
        [(latent_rows * growth * second_half - 1.0) * scale_inv, latent_rows * scale_inv], axis=-1
    ).astype(jnp.bfloat16)
    end_grad = jnp.einsum("cti,ctg->ig", skip_b, grad_out, preferred_element_type=jnp.float32)
    skip_back = jnp.einsum(
        "ctg,ig->cti", grad_out, end_weight, preferred_element_type=jnp.float32
    ).astype(jnp.bfloat16)
    state_back = jnp.zeros((clips_dev, frames_dev, channels), jnp.float32)
    in_grads = [None] * layers
    cond_grads = [None] * layers
    res_grads = [None] * (layers - 1)
    last_grad = None
    clip_sums = [None] * layers
    dp_size = lax.axis_size("dp")
    tm_size = lax.axis_size("tm")

    def by_clip_owner(grad):
        return grad.astype(jnp.bfloat16).reshape(dp_size, -1, grad.shape[1])

    def folded(grad):
        rows, columns = grad.shape
        halves = grad.astype(jnp.bfloat16).reshape(dp_size, 2, rows // dp_size // 2, columns)
        return jnp.transpose(halves, (0, 2, 1, 3)).reshape(rows // 2, 2 * columns)

    def unfolded(grad):
        rows, columns = grad.shape
        halves = grad.reshape(dp_size, rows // dp_size, 2, columns // 2)
        return jnp.transpose(halves, (0, 2, 1, 3)).reshape(2 * rows, columns // 2)

    for layer_index in reversed(range(layers)):
        spread = 2**layer_index
        padded, pre_act, gated_out = stored[layer_index]
        if layer_index == layers - 1:
            act_back = jnp.einsum(
                "ctj,ij->cti", skip_back, last_weight, preferred_element_type=jnp.float32
            )
            last_grad = jnp.einsum(
                "cti,ctj->ij", gated_out, skip_back, preferred_element_type=jnp.float32
            )
        else:
            joined = jnp.concatenate([state_back.astype(jnp.bfloat16), skip_back], axis=-1)
            act_back = jnp.einsum(
                "ctj,ij->cti", joined, res_weight[layer_index], preferred_element_type=jnp.float32
            )
            res_grads[layer_index] = jnp.einsum(
                "cti,ctj->ij", gated_out, joined, preferred_element_type=jnp.float32
            )
        pre_back = gated_back(pre_act, act_back, channels).astype(jnp.bfloat16)
        in_grads[layer_index] = [
                jnp.einsum(
                    "cti,cto->io",
                    padded[:, tap_index * spread : tap_index * spread + frames_dev],
                    pre_back,
                    preferred_element_type=jnp.float32,
                )
                for tap_index in range(taps)
            ]
        cond_grads[layer_index] = jnp.einsum(
            "ctm,cto->mo", mel_frames, pre_back, preferred_element_type=jnp.float32
        )
        grad_pad = with_halo(pre_back, (("tm", 1),), spread)
        state_back = state_back + dilated_back(
            grad_pad, input_weight[layer_index], spread, frames_dev
        )
        pieces = in_grads[layer_index] + [cond_grads[layer_index]]
        if layer_index == layers - 1:
            pieces.append(folded(last_grad))
        else:
            pieces.append(res_grads[layer_index])
        packed = jnp.concatenate([by_clip_owner(piece) for piece in pieces], axis=1)
        packed = with_layout_constraint(packed, Layout(major_to_minor=(0, 1, 2)))
        clip_sums[layer_index] = lax.psum_scatter(
            packed, "dp", scatter_dimension=0, tiled=True
        )[0]
    start_grad = jnp.einsum("cth,ctk->hk", first_half, state_back, precision=highest)
    first_back = (
        jnp.einsum("ctk,hk->cth", state_back, start_weight, precision=highest)
        + first_half * scale_inv
    )
    audio_grad = jnp.transpose(
        jnp.concatenate([first_back, latent_rows * growth * scale_inv], axis=-1), (0, 2, 1)
    )
    latent = jnp.transpose(latent_rows, (0, 2, 1))
    small = jnp.concatenate(
        [end_grad.reshape(-1), start_grad.reshape(-1), local_loss.reshape(1)]
    )
    small = lax.psum(lax.psum(small, "tm"), "dp")
    end_total = small[: end_grad.size].reshape(end_grad.shape)
    start_total = small[end_grad.size : end_grad.size + start_grad.size].reshape(start_grad.shape)
    batch_loss = small[-1]
    grad_rows = clip_sums[-1].shape[0] - channels // dp_size // 2
    last_parts = lax.all_gather(clip_sums[-1][grad_rows:], "tm")
    last_rows = jnp.sum(last_parts.astype(jnp.float32), axis=0).astype(jnp.bfloat16)
    last_total = unfolded(lax.all_gather(last_rows, "dp", tiled=True)).astype(jnp.float32)
    clip_sums = clip_sums[:-1] + [clip_sums[-1][:grad_rows]]
    clip_sums, end_total, start_total, batch_loss, last_total = lax.optimization_barrier(
        (clip_sums, end_total, start_total, batch_loss, last_total)
    )
    rows_all = jnp.concatenate(clip_sums, axis=0)
    width = rows_all.shape[1] // tm_size
    by_frame_owner = jnp.stack(
        [rows_all[:, at * width : (at + 1) * width] for at in range(tm_size)]
    )
    by_frame_owner = with_layout_constraint(by_frame_owner, Layout(major_to_minor=(0, 1, 2)))
    mine = lax.psum_scatter(by_frame_owner, "tm", scatter_dimension=0, tiled=True)[0]
    mine = mine.astype(jnp.float32)
    in_sums, cond_sums, res_sums, taken = [], [], [], 0
    for layer_index in range(layers):
        rows = taps * channels // dp_size
        in_sums.append(mine[taken : taken + rows].reshape(taps, channels // dp_size, width))
        taken += rows
        rows = mel_frames.shape[2] // dp_size
        cond_sums.append(mine[taken : taken + rows])
        taken += rows
        if layer_index < layers - 1:
            rows = channels // dp_size
            res_sums.append(mine[taken : taken + rows])
            taken += rows
    in_grad = jnp.stack(in_sums)
    cond_grad = jnp.stack(cond_sums)
    res_grad = jnp.stack(res_sums)
    return (
        latent,
        audio_grad,
        batch_loss,
        in_grad,
        cond_grad,
        res_grad,
        last_total,
        end_total,
        start_total,
    )


def solution(mesh):
    return jax.shard_map(
        shards,
        mesh=mesh,
        in_specs=(P("dp", None, "tm"), P("dp", "tm", None), P(), P(), P(), P(), P(), P()),
        out_specs=(
            P("dp", None, "tm"),
            P("dp", None, "tm"),
            P(),
            P(None, None, "dp", "tm"),
            P(None, "dp", "tm"),
            P(None, "dp", "tm"),
            P(),
            P(),
            P(),
        ),
        check_vma=False,
    )
```
